256 devices in a mesh: seq: 32 (over y, z), head: 8 (over x, core).
Axes of the slice: x: 4, y: 4, z: 8, core: 2. Of those that a mesh axis runs over, the one named last changes fastest.
Arguments:
- doc_lengths: int32 [256], P(('seq', 'head')), may hold values from 1 to 2688, 24576 in all
- queries: bfloat16 [24576, 8192], P('seq', 'head'), may hold values from -24 to 24
- key_states: bfloat16 [24576, 1024], P('seq', 'head'), may hold values from -24 to 24
- value_states: bfloat16 [24576, 1024], P('seq', 'head'), may hold values from -6 to 6
Outputs:
- attended: bfloat16 [24576, 8192], P('seq', 'head')
The draws below stay inside these ranges and needn't reach their ends.
Inputs may be any that keep to these rules, and one draw needn't show every extreme that they name: `doc_lengths`: the 256 lengths sum to 24576; the largest is exactly 2688.
All inputs are finite; a program needn't handle non-finite values. No bound on the sum of `doc_lengths` on one device may be relied on, other than what follows from the above.
Results may differ from the reference program's by a relative error of at most 0.0028.
Values may be sent and summed in bfloat16 or wider, within the bound.
No kernel may reach another device: no remote copies, remote signals or barrier semaphores. Data moves between devices by JAX's collectives and lax.ppermute only.
A program may use at most 64 MiB of HBM per device.

```python
import math
import jax
import jax.numpy as jnp
import numpy as np
from jax import lax

HD = 128
QH = 64
KVH = 8
TILE = 128
GROUP = 8
TOKENS = 24576
DOCS = 256
LONGEST = 2688


def draw_queries(key, part):
    drawn = jnp.clip(jax.random.normal(jax.random.fold_in(key, 1), (TOKENS, QH * HD)), -6.0, 6.0)
    return drawn.astype(jnp.bfloat16)


def draw_key_states(key, part):
    drawn = jnp.clip(jax.random.normal(jax.random.fold_in(key, 2), (TOKENS, KVH * HD)), -6.0, 6.0)
    return drawn.astype(jnp.bfloat16)


def shard_levels(rng, shape, cuts, smallest, top_value):
    def one(dim, shards_of):
        steps = jax.random.uniform(jax.random.fold_in(jax.random.fold_in(rng, 6), dim), (shards_of,), jnp.float32, smallest / len(cuts), top_value / len(cuts))
        return jnp.repeat(jnp.exp(steps), shape[dim] // shards_of).reshape((-1,) + (1,) * (len(shape) - dim - 1))

    gain = one(*cuts[0])
    for cut in cuts[1:]:
        gain = gain * one(*cut)
    return gain


def length_profile(number_of, total, bound, skew):
    weights = [(1 << 20) // math.isqrt(grade ** skew) + 1 for grade in range(2, number_of + 1)]
    rest, counts = total - bound - (number_of - 1), [1] * (number_of - 1)
    while rest > 0:
        candidates = [i for i in range(number_of - 1) if counts[i] < bound]
        whole, remaining = sum([weights[i] for i in candidates]), rest
        for i in candidates:
            extra = min(bound - counts[i], max(1, remaining * weights[i] // whole), rest)
            counts[i] = counts[i] + extra
            rest = rest - extra
    return np.array([bound] + counts)


def ragged(rng, number_of, total, most, skew):
    if number_of == 2:
        one = jax.random.randint(rng, (), max(1, total - most), min(most, total - 1) + 1)
        return jnp.stack([one, total - one])
    tallies = jnp.asarray(length_profile(number_of, total, most, skew), jnp.int32)
    pairs = (number_of - 1) // 2
    giver, taker = tallies[1:1 + 2 * pairs:2], tallies[2:2 + 2 * pairs:2]
    slack = jnp.minimum(giver - 1, most - taker)
    shifted = jax.random.randint(jax.random.fold_in(rng, 1), (pairs,), 0, 1 << 20) % (slack + 1)
    tallies = tallies.at[1:1 + 2 * pairs:2].set(giver - shifted).at[2:2 + 2 * pairs:2].set(taker + shifted)
    return tallies[jax.random.permutation(jax.random.fold_in(rng, 2), number_of)]


def centred(stream_key, shape, deviation, reach, pieces=(), kind=jnp.bfloat16):
    level = shard_levels(stream_key, shape, pieces, -0.22, 0.18) if pieces else 1.0
    values = jax.random.normal(stream_key, shape, jnp.float32) * deviation * level
    return jnp.minimum(jnp.maximum(values, -reach), reach).astype(kind)


def setup_inputs(seed: int = 0) -> dict:
    splits = jax.random.split(jax.random.key(seed), 5)
    return {
        "doc_lengths": ragged(splits[0], DOCS, TOKENS, LONGEST, 2).astype(jnp.int32),
        "queries": draw_queries(jax.random.fold_in(splits[4], 71), 0),
        "key_states": draw_key_states(jax.random.fold_in(splits[4], 71), 0),
        "value_states": centred(splits[3], (TOKENS, KVH * HD), 1.0, 6.0, ((0, 32), (1, 8))),
    }


far_below = -1e+30

def document_start(positions, doc_ends, doc_lengths):
    finished = doc_ends[None, :] <= positions[:, None]
    return lax.optimization_barrier(jnp.sum(jnp.where(finished, doc_lengths[None, :], 0), axis=1)).astype(jnp.int32)

def reference(doc_lengths, queries, key_states, value_states):
    doc_ends = jnp.cumsum(doc_lengths).astype(jnp.int32)
    key_span = LONGEST + TILE
    front_zeros = jnp.zeros((LONGEST, KVH * HD), key_states.dtype)
    padded_keys = jnp.concatenate([front_zeros, key_states], axis=0)
    padded_values = jnp.concatenate([front_zeros, value_states], axis=0)
    score_scale = 1.0 / math.sqrt(HD)

    def one_tile(tile_index):
        first_row = (tile_index * TILE).astype(jnp.int32)
        query_tile = lax.dynamic_slice_in_dim(queries, first_row, TILE, 0).reshape(TILE, KVH, GROUP, HD).astype(jnp.float32)
        key_window = lax.dynamic_slice_in_dim(padded_keys, first_row, key_span, 0).reshape(key_span, KVH, HD).astype(jnp.float32)
        value_window = lax.dynamic_slice_in_dim(padded_values, first_row, key_span, 0).reshape(key_span, KVH, HD).astype(jnp.float32)
        query_pos = first_row + jnp.arange(TILE, dtype=jnp.int32)
        key_pos = first_row - LONGEST + jnp.arange(key_span, dtype=jnp.int32)
        starts = document_start(query_pos, doc_ends, doc_lengths)
        visible = (key_pos[None, :] >= starts[:, None]) & (key_pos[None, :] <= query_pos[:, None])
        scores = jnp.einsum('qhgd,khd->hgqk', query_tile, key_window) * score_scale
        scores = jnp.where(visible, scores, far_below)
        row_max = lax.optimization_barrier(jnp.max(scores, axis=-1, keepdims=True))
        weights = jnp.where(visible, jnp.exp(scores - row_max), 0.0)
        weight_sum = lax.optimization_barrier(jnp.sum(weights, axis=-1, keepdims=True))
        rounded = lax.optimization_barrier(weights.astype(jnp.bfloat16))
        mixed_out = jnp.einsum('hgqk,khd->hgqd', rounded.astype(jnp.float32), value_window) / weight_sum
        return mixed_out.transpose(2, 0, 1, 3).reshape(TILE, QH * HD).astype(jnp.bfloat16)
    all_tiles = lax.map(one_tile, jnp.arange(TOKENS // TILE, dtype=jnp.int32))
    return all_tiles.reshape(TOKENS, QH * HD)
```

```python
import math

import jax
import jax.numpy as jnp
from jax import lax
from jax.experimental import pallas as pl
from jax.experimental.pallas import tpu as pltpu
from jax.sharding import Mesh
from jax.sharding import PartitionSpec as P

SEQ = ("seq_0", "seq_1")
HEAD = ("head_0", "head_1")

HD = 128
TILE = 128
KB = 384
HEADS_PER_DOT = 8
VL = 30
FAR_BELOW = -1e30
EXP2_SCALE = math.log2(math.e) / math.sqrt(HD)
NT = (((1,), (1,)), ((), ()))
NN = (((1,), (0,)), ((), ()))


def tile_starts(lengths_ref, ends_ref, first_pos):
    ends = ends_ref[...]
    pos = first_pos + lax.broadcasted_iota(jnp.int32, (TILE, ends.shape[1]), 0)
    return jnp.max(jnp.where(ends <= pos, ends, 0), axis=1, keepdims=True)


def fill_ends(lengths_ref, ends_ref):
    docs = lengths_ref.shape[0]
    lengths = lengths_ref[...]
    order = lax.broadcasted_iota(jnp.int32, lengths.shape, 0)
    lane = lax.broadcasted_iota(jnp.int32, lengths.shape, 1)
    for part in range(docs // 128):
        kept = jnp.where(order <= lane + part * 128, lengths, 0)
        ends_ref[:, part * 128 : (part + 1) * 128] = jnp.sum(kept, axis=0, keepdims=True)


def accumulate(qs_ref, kv_ref, row, mask, m_ref, l_ref, acc_ref, fresh):
    rows_all = qs_ref.shape[0]
    step = HEADS_PER_DOT * TILE
    keys = kv_ref[pl.ds(row, KB), :HD]
    values = kv_ref[pl.ds(row, KB), HD:]
    for first in range(0, rows_all, step):
        rows = slice(first, first + step)
        scores = lax.dot_general(qs_ref[rows], keys, NT, preferred_element_type=jnp.float32)
        if mask is not None:
            scores = jnp.where(mask, scores.reshape(HEADS_PER_DOT, TILE, KB), FAR_BELOW).reshape(step, KB)
        top = jnp.max(scores, axis=1, keepdims=True)
        if not fresh:
            old = m_ref[rows]
            new = jnp.maximum(old, top)
            shrink = jnp.exp2((old - new) * EXP2_SCALE)
        else:
            new = jnp.broadcast_to(top, (step, 128))
        m_ref[rows] = new
        parts = [
            jnp.exp2((scores[:, c : c + 128] - new) * EXP2_SCALE) for c in range(0, KB, 128)
        ]
        total = parts[0]
        for part in parts[1:]:
            total = total + part
        weights = jnp.concatenate([part.astype(jnp.bfloat16) for part in parts], axis=1)
        update = lax.dot_general(weights, values, NN, preferred_element_type=jnp.float32)
        if not fresh:
            total = total + l_ref[rows] * shrink
            update = update + acc_ref[rows] * shrink
        l_ref[rows] = total
        acc_ref[rows] = update


def visible(first_pos, key_pos, starts, diagonal):
    key = key_pos + lax.broadcasted_iota(jnp.int32, (TILE, KB), 1)
    seen = key >= starts
    if diagonal:
        seen = seen & (key <= first_pos + lax.broadcasted_iota(jnp.int32, (TILE, KB), 0))
    return seen


def near_kernel(base_ref, lengths_ref, q_ref, kv0_ref, kv1_ref, kv2_ref,
                m_out, l_out, acc_out, kv_ref, qs_ref, ends_ref, sems):
    tok = kv0_ref.shape[0]
    copies = [
        pltpu.make_async_copy(src, kv_ref.at[pl.ds(i * tok, tok)], sems.at[i])
        for i, src in enumerate((kv2_ref, kv1_ref, kv0_ref))
    ]
    for copy in copies:
        copy.start()
    fill_ends(lengths_ref, ends_ref)
    base = base_ref[0]
    kv_base = base - 2 * tok
    for copy in copies:
        copy.wait()
    heads = q_ref.shape[1] // HD

    def tile(t, _):
        first_pos = base + t * TILE
        starts = tile_starts(lengths_ref, ends_ref, first_pos)
        low = jnp.min(starts)
        high = jnp.max(starts)
        q_rows = pl.multiple_of(t * TILE, TILE)
        for h in range(heads):
            qs_ref[h * TILE : (h + 1) * TILE, :] = q_ref[pl.ds(q_rows, TILE), h * HD : (h + 1) * HD]
        m_ref, l_ref, acc_ref = m_out.at[t], l_out.at[t], acc_out.at[t]
        last = (2 * tok + t * TILE) // KB
        lowest = jnp.maximum(low - kv_base, 0) // KB
        row = pl.multiple_of(last * KB, KB)
        mask = visible(first_pos, kv_base + row, starts, True)
        accumulate(qs_ref, kv_ref, row, mask, m_ref, l_ref, acc_ref, True)

        def block(i, _):
            row = pl.multiple_of((last - 1 - i) * KB, KB)
            key_pos = kv_base + row

            @pl.when(key_pos >= high)
            def _():
                accumulate(qs_ref, kv_ref, row, None, m_ref, l_ref, acc_ref, False)

            @pl.when(key_pos < high)
            def _():
                mask = visible(first_pos, key_pos, starts, False)
                accumulate(qs_ref, kv_ref, row, mask, m_ref, l_ref, acc_ref, False)

            return 0

        lax.fori_loop(0, last - lowest, block, 0)
        return 0

    lax.fori_loop(0, q_ref.shape[0] // TILE, tile, 0)


def far_kernel(base_ref, lengths_ref, q_ref, kv3_ref, kv4_ref, m_in, l_in, acc_in,
               out_ref, kv_ref, qs_ref, ends_ref, m_ref, l_ref, acc_ref, sems):
    tok = kv3_ref.shape[0]
    half = kv4_ref.shape[0]
    pad = kv_ref.shape[0] - tok - half
    copies = [
        pltpu.make_async_copy(kv4_ref, kv_ref.at[pl.ds(pad, half)], sems.at[0]),
        pltpu.make_async_copy(kv3_ref, kv_ref.at[pl.ds(pad + half, tok)], sems.at[1]),
    ]
    for copy in copies:
        copy.start()
    if pad:
        kv_ref[:pad, :] = jnp.zeros((pad, kv_ref.shape[1]), kv_ref.dtype)
    fill_ends(lengths_ref, ends_ref)
    base = base_ref[0]
    top_pos = base - 2 * tok
    kv_base = top_pos - tok - half - pad
    for copy in copies:
        copy.wait()
    heads = q_ref.shape[1] // HD
    count = kv_ref.shape[0] // KB

    def tile(t, _):
        first_pos = base + t * TILE
        starts = tile_starts(lengths_ref, ends_ref, first_pos)
        low = jnp.min(starts)
        high = jnp.max(starts)
        q_rows = pl.multiple_of(t * TILE, TILE)

        def finish(m_now, l_now, acc_now):
            for h in range(heads):
                rows = slice(h * TILE, (h + 1) * TILE)
                total = jnp.sum(l_now[rows], axis=1, keepdims=True)
                out_ref[pl.ds(q_rows, TILE), h * HD : (h + 1) * HD] = (
                    acc_now[rows] * (1.0 / total)
                ).astype(out_ref.dtype)

        @pl.when(low >= top_pos)
        def _():
            finish(m_in.at[t], l_in.at[t], acc_in.at[t])

        @pl.when(low < top_pos)
        def _():
            for h in range(heads):
                qs_ref[h * TILE : (h + 1) * TILE, :] = q_ref[pl.ds(q_rows, TILE), h * HD : (h + 1) * HD]
            m_ref[...] = m_in[t]
            l_ref[...] = l_in[t]
            acc_ref[...] = acc_in[t]
            lowest = jnp.maximum(low - kv_base, 0) // KB

            def block(i, _):
                row = pl.multiple_of((count - 1 - i) * KB, 128)
                key_pos = kv_base + row

                @pl.when(key_pos >= high)
                def _():
                    accumulate(qs_ref, kv_ref, row, None, m_ref, l_ref, acc_ref, False)

                @pl.when(key_pos < high)
                def _():
                    mask = visible(first_pos, key_pos, starts, False)
                    accumulate(qs_ref, kv_ref, row, mask, m_ref, l_ref, acc_ref, False)

                return 0

            lax.fori_loop(0, count - lowest, block, 0)
            finish(m_ref, l_ref, acc_ref)

        return 0

    lax.fori_loop(0, q_ref.shape[0] // TILE, tile, 0)


VM = pl.BlockSpec(memory_space=pltpu.VMEM)
SM = pl.BlockSpec(memory_space=pltpu.SMEM)
ANY = pl.BlockSpec(memory_space=pl.ANY)


def near(base, lengths, q, kv0, kv1, kv2):
    tok, width = q.shape
    tiles, rows = tok // TILE, width // HD * TILE
    state = jax.ShapeDtypeStruct((tiles, rows, 128), jnp.float32)
    return pl.pallas_call(
        near_kernel,
        out_shape=(state,) * 3,
        in_specs=[SM, VM, VM, ANY, ANY, ANY],
        out_specs=(VM,) * 3,
        scratch_shapes=[
            pltpu.VMEM((3 * tok, 2 * HD), jnp.bfloat16),
            pltpu.VMEM((rows, HD), jnp.bfloat16),
            pltpu.VMEM((1, lengths.shape[0]), jnp.int32),
            pltpu.SemaphoreType.DMA((3,)),
        ],
        compiler_params=pltpu.CompilerParams(vmem_limit_bytes=VL << 20),
        cost_estimate=pl.CostEstimate(flops=8_000_000_000, bytes_accessed=16 << 20, transcendentals=0),
        name="near",
    )(base, lengths, q, kv0, kv1, kv2)


def far(base, lengths, q, kv3, kv4, m, l, acc):
    tok, width = q.shape
    rows = width // HD * TILE
    return pl.pallas_call(
        far_kernel,
        out_shape=jax.ShapeDtypeStruct(q.shape, q.dtype),
        in_specs=[SM, VM, VM, ANY, ANY, VM, VM, VM],
        out_specs=VM,
        scratch_shapes=[
            pltpu.VMEM((-(-(tok + tok // 2) // KB) * KB, 2 * HD), jnp.bfloat16),
            pltpu.VMEM((rows, HD), jnp.bfloat16),
            pltpu.VMEM((1, lengths.shape[0]), jnp.int32),
            pltpu.VMEM((rows, 128), jnp.float32),
            pltpu.VMEM((rows, 128), jnp.float32),
            pltpu.VMEM((rows, 128), jnp.float32),
            pltpu.SemaphoreType.DMA((2,)),
        ],
        compiler_params=pltpu.CompilerParams(vmem_limit_bytes=VL << 20),
        cost_estimate=pl.CostEstimate(flops=2_000_000_000, bytes_accessed=16 << 20, transcendentals=0),
        name="far",
    )(base, lengths, q, kv3, kv4, m, l, acc)


def from_behind(value, steps):
    count = lax.axis_size(SEQ)
    return lax.ppermute(value, SEQ, [(source, source + steps) for source in range(count - steps)])


def all_lengths(doc_lengths):
    heads, shards = lax.axis_size(HEAD), lax.axis_size(SEQ)
    per_head = doc_lengths.shape[0]
    rows = heads * per_head
    order = lax.broadcasted_iota(jnp.int32, (rows, 128), 0)
    mine = jnp.zeros((rows, 128), jnp.int32)
    for i in range(per_head):
        mine = jnp.where(order == lax.axis_index(HEAD) * per_head + i, doc_lengths[i], mine)
    group = lax.psum(mine, HEAD)
    spread = jnp.broadcast_to(group[None], (shards, rows, 128))
    return lax.all_to_all(spread, SEQ, 0, 0, tiled=True).reshape(shards * rows, 128)


def body(doc_lengths, queries, key_states, value_states):
    tok = queries.shape[0]
    own = jnp.concatenate([key_states, value_states], axis=1)
    lengths = all_lengths(doc_lengths)
    one = from_behind(own, 1)
    two = from_behind(one, 1)
    three = from_behind(two, 1)
    four = from_behind(two[tok // 2 :], 2)
    base = jnp.reshape(lax.axis_index(SEQ) * tok, (1,)).astype(jnp.int32)
    m, l, acc = near(base, lengths, queries, own, one, two)
    return far(base, lengths, queries, three, four, m, l, acc)


def solution(mesh):
    finer = Mesh(mesh.devices.reshape(4, 8, 4, 2), SEQ + HEAD)
    return jax.shard_map(
        body,
        mesh=finer,
        in_specs=(P(SEQ + HEAD), P(SEQ, HEAD), P(SEQ, HEAD), P(SEQ, HEAD)),
        out_specs=P(SEQ, HEAD),
        check_vma=False,
    )
```

```python
import math

import jax
import jax.numpy as jnp
from jax import lax
from jax.experimental import pallas as pl
from jax.experimental.pallas import tpu as pltpu
from jax.sharding import Mesh
from jax.sharding import PartitionSpec as P

SEQ = ("seq_0", "seq_1")
HEAD = ("head_0", "head_1")

HD = 128
TILE = 128
KB = 384
HEADS_PER_DOT = 8
VL = 30
FAR_BELOW = -1e30
EXP2_SCALE = math.log2(math.e) / math.sqrt(HD)
NT = (((1,), (1,)), ((), ()))
NN = (((1,), (0,)), ((), ()))


def fill_ends(lengths_ref, ends_ref):
    docs = lengths_ref.shape[0]
    lengths = lengths_ref[...]
    order = lax.broadcasted_iota(jnp.int32, lengths.shape, 0)
    lane = lax.broadcasted_iota(jnp.int32, lengths.shape, 1)
    for part in range(docs // 128):
        kept = jnp.where(order <= lane + part * 128, lengths, 0)
        ends_ref[:, part * 128 : (part + 1) * 128] = jnp.sum(kept, axis=0, keepdims=True)


def place_tiles(base, lengths_ref, ends_ref, starts_ref, low_ref, high_ref):
    fill_ends(lengths_ref, ends_ref)
    ends = ends_ref[...]
    for t in range(starts_ref.shape[0]):
        pos = base + t * TILE + lax.broadcasted_iota(jnp.int32, (TILE, ends.shape[1]), 0)
        starts = jnp.max(jnp.where(ends <= pos, ends, 0), axis=1, keepdims=True)
        starts_ref[t] = jnp.broadcast_to(starts, (TILE, 128))
        low_ref[t] = jnp.min(starts)
        high_ref[t] = jnp.max(starts)


def take_tile(q_ref, t, qs_ref):
    rows = pl.ds(pl.multiple_of(t * TILE, TILE), TILE)
    for h in range(q_ref.shape[1] // HD):
        qs_ref[h * TILE : (h + 1) * TILE, :] = q_ref[rows, h * HD : (h + 1) * HD]


def accumulate(qs_ref, k_ref, v_ref, row, mask, m_ref, l_ref, acc_ref, fresh):
    rows_all = qs_ref.shape[0]
    step = HEADS_PER_DOT * TILE
    keys = k_ref[pl.ds(row, KB), :]
    values = v_ref[pl.ds(row, KB), :]
    for first in range(0, rows_all, step):
        rows = slice(first, first + step)
        scores = lax.dot_general(qs_ref[rows], keys, NT, preferred_element_type=jnp.float32)
        if mask is not None:
            scores = jnp.where(mask, scores.reshape(HEADS_PER_DOT, TILE, KB), FAR_BELOW).reshape(step, KB)
        top = jnp.max(scores, axis=1, keepdims=True)
        if not fresh:
            old = m_ref[rows]
            new = jnp.maximum(old, top)
            shrink = jnp.exp2((old - new) * EXP2_SCALE)
        else:
            new = jnp.broadcast_to(top, (step, 128))
        m_ref[rows] = new
        parts = [
            jnp.exp2((scores[:, c : c + 128] - new) * EXP2_SCALE) for c in range(0, KB, 128)
        ]
        total = parts[0]
        for part in parts[1:]:
            total = total + part
        weights = jnp.concatenate([part.astype(jnp.bfloat16) for part in parts], axis=1)
        update = lax.dot_general(weights, values, NN, preferred_element_type=jnp.float32)
        if not fresh:
            total = total + l_ref[rows] * shrink
            update = update + acc_ref[rows] * shrink
        l_ref[rows] = total
        acc_ref[rows] = update


def visible(first_pos, key_pos, starts, diagonal):
    key = key_pos + lax.broadcasted_iota(jnp.int32, (TILE, KB), 1)
    seen = key >= starts
    if diagonal:
        seen = seen & (key <= first_pos + lax.broadcasted_iota(jnp.int32, (TILE, KB), 0))
    return seen


def spread_copies(blocks, k_ref, v_ref, sems):
    copies = []
    for i, (src, row) in enumerate(blocks):
        rows = pl.ds(row, src.shape[1])
        copies += [
            pltpu.make_async_copy(src.at[0], k_ref.at[rows], sems.at[2 * i]),
            pltpu.make_async_copy(src.at[1], v_ref.at[rows], sems.at[2 * i + 1]),
        ]
    return copies


def near_kernel(base_ref, lengths_ref, q_ref, kv0_ref, kv1_ref, kv2_ref,
                m_out, l_out, acc_out, k_ref, v_ref, qs_ref, ends_ref, starts_ref, low_ref, high_ref, sems):
    tok = kv0_ref.shape[1]
    copies = spread_copies(
        [(kv2_ref, 0), (kv1_ref, tok), (kv0_ref, 2 * tok)], k_ref, v_ref, sems
    )
    for copy in copies:
        copy.start()
    base = base_ref[0]
    place_tiles(base, lengths_ref, ends_ref, starts_ref, low_ref, high_ref)
    kv_base = base - 2 * tok
    for copy in copies:
        copy.wait()

    def tile(t, _):
        first_pos = base + t * TILE
        low = low_ref[t]
        high = high_ref[t]
        take_tile(q_ref, t, qs_ref)
        m_ref, l_ref, acc_ref = m_out.at[t], l_out.at[t], acc_out.at[t]
        last = (2 * tok + t * TILE) // KB
        lowest = jnp.maximum(low - kv_base, 0) // KB
        row = pl.multiple_of(last * KB, KB)
        mask = visible(first_pos, kv_base + row, starts_ref[t][:, :1], True)
        accumulate(qs_ref, k_ref, v_ref, row, mask, m_ref, l_ref, acc_ref, True)

        def block(i, _):
            row = pl.multiple_of((last - 1 - i) * KB, KB)
            key_pos = kv_base + row

            @pl.when(key_pos >= high)
            def _():
                accumulate(qs_ref, k_ref, v_ref, row, None, m_ref, l_ref, acc_ref, False)

            @pl.when(key_pos < high)
            def _():
                mask = visible(first_pos, key_pos, starts_ref[t][:, :1], False)
                accumulate(qs_ref, k_ref, v_ref, row, mask, m_ref, l_ref, acc_ref, False)

            return 0

        lax.fori_loop(0, last - lowest, block, 0)
        return 0

    lax.fori_loop(0, q_ref.shape[0] // TILE, tile, 0)


def far_kernel(base_ref, lengths_ref, q_ref, kv3_ref, kv4_ref, m_in, l_in, acc_in,
               out_ref, k_ref, v_ref, qs_ref, ends_ref, starts_ref, low_ref, high_ref, m_ref, l_ref, acc_ref, sems):
    tok = kv3_ref.shape[1]
    half = kv4_ref.shape[1]
    copies = spread_copies([(kv4_ref, 0), (kv3_ref, half)], k_ref, v_ref, sems)
    for copy in copies:
        copy.start()
    base = base_ref[0]
    place_tiles(base, lengths_ref, ends_ref, starts_ref, low_ref, high_ref)
    top_pos = base - 2 * tok
    kv_base = top_pos - tok - half
    for copy in copies:
        copy.wait()
    heads = q_ref.shape[1] // HD
    count = k_ref.shape[0] // KB

    def tile(t, _):
        first_pos = base + t * TILE
        low = low_ref[t]
        high = high_ref[t]
        q_rows = pl.multiple_of(t * TILE, TILE)

        def finish(m_now, l_now, acc_now):
            for h in range(heads):
                rows = slice(h * TILE, (h + 1) * TILE)
                total = jnp.sum(l_now[rows], axis=1, keepdims=True)
                out_ref[pl.ds(q_rows, TILE), h * HD : (h + 1) * HD] = (
                    acc_now[rows] * (1.0 / total)
                ).astype(out_ref.dtype)

        @pl.when(low >= top_pos)
        def _():
            finish(m_in.at[t], l_in.at[t], acc_in.at[t])

        @pl.when(low < top_pos)
        def _():
            take_tile(q_ref, t, qs_ref)
            m_ref[...] = m_in[t]
            l_ref[...] = l_in[t]
            acc_ref[...] = acc_in[t]
            lowest = jnp.maximum(low - kv_base, 0) // KB

            def block(i, _):
                row = pl.multiple_of((count - 1 - i) * KB, KB)
                key_pos = kv_base + row

                @pl.when(key_pos >= high)
                def _():
                    accumulate(qs_ref, k_ref, v_ref, row, None, m_ref, l_ref, acc_ref, False)

                @pl.when(key_pos < high)
                def _():
                    mask = visible(first_pos, key_pos, starts_ref[t][:, :1], False)
                    accumulate(qs_ref, k_ref, v_ref, row, mask, m_ref, l_ref, acc_ref, False)

                return 0

            lax.fori_loop(0, count - lowest, block, 0)
            finish(m_ref, l_ref, acc_ref)

        return 0

    lax.fori_loop(0, q_ref.shape[0] // TILE, tile, 0)


VM = pl.BlockSpec(memory_space=pltpu.VMEM)
SM = pl.BlockSpec(memory_space=pltpu.SMEM)
ANY = pl.BlockSpec(memory_space=pl.ANY)


def near(base, lengths, q, kv0, kv1, kv2):
    tok, width = q.shape
    tiles, rows = tok // TILE, width // HD * TILE
    state = jax.ShapeDtypeStruct((tiles, rows, 128), jnp.float32)
    return pl.pallas_call(
        near_kernel,
        out_shape=(state,) * 3,
        in_specs=[SM, VM, VM, ANY, ANY, ANY],
        out_specs=(VM,) * 3,
        scratch_shapes=[
            pltpu.VMEM((3 * tok, HD), jnp.bfloat16),
            pltpu.VMEM((3 * tok, HD), jnp.bfloat16),
            pltpu.VMEM((rows, HD), jnp.bfloat16),
            pltpu.VMEM((1, lengths.shape[0]), jnp.int32),
            pltpu.VMEM((tok // TILE, TILE, 128), jnp.int32),
            pltpu.SMEM((tok // TILE,), jnp.int32),
            pltpu.SMEM((tok // TILE,), jnp.int32),
            pltpu.SemaphoreType.DMA((6,)),
        ],
        compiler_params=pltpu.CompilerParams(vmem_limit_bytes=VL << 20),
        cost_estimate=pl.CostEstimate(flops=8_000_000_000, bytes_accessed=16 << 20, transcendentals=0),
        name="near",
    )(base, lengths, q, kv0, kv1, kv2)


def far(base, lengths, q, kv3, kv4, m, l, acc):
    tok, width = q.shape
    rows = width // HD * TILE
    return pl.pallas_call(
        far_kernel,
        out_shape=jax.ShapeDtypeStruct(q.shape, q.dtype),
        in_specs=[SM, VM, VM, ANY, ANY, VM, VM, VM],
        out_specs=VM,
        scratch_shapes=[
            pltpu.VMEM((tok + tok // 2, HD), jnp.bfloat16),
            pltpu.VMEM((tok + tok // 2, HD), jnp.bfloat16),
            pltpu.VMEM((rows, HD), jnp.bfloat16),
            pltpu.VMEM((1, lengths.shape[0]), jnp.int32),
            pltpu.VMEM((tok // TILE, TILE, 128), jnp.int32),
            pltpu.SMEM((tok // TILE,), jnp.int32),
            pltpu.SMEM((tok // TILE,), jnp.int32),
            pltpu.VMEM((rows, 128), jnp.float32),
            pltpu.VMEM((rows, 128), jnp.float32),
            pltpu.VMEM((rows, 128), jnp.float32),
            pltpu.SemaphoreType.DMA((4,)),
        ],
        compiler_params=pltpu.CompilerParams(vmem_limit_bytes=VL << 20),
        cost_estimate=pl.CostEstimate(flops=2_000_000_000, bytes_accessed=16 << 20, transcendentals=0),
        name="far",
    )(base, lengths, q, kv3, kv4, m, l, acc)


def from_behind(value, steps):
    count = lax.axis_size(SEQ)
    return lax.ppermute(value, SEQ, [(source, source + steps) for source in range(count - steps)])


def head_lengths(doc_lengths):
    heads = lax.axis_size(HEAD)
    per_head = doc_lengths.shape[0]
    rows = heads * per_head
    order = lax.broadcasted_iota(jnp.int32, (rows, 128), 0)
    mine = jnp.zeros((rows, 128), jnp.int32)
    for i in range(per_head):
        mine = jnp.where(order == lax.axis_index(HEAD) * per_head + i, doc_lengths[i], mine)
    return lax.psum(mine, HEAD)


def all_lengths(group):
    shards = lax.axis_size(SEQ)
    spread = jnp.broadcast_to(group[None], (shards, *group.shape))
    return lax.all_to_all(spread, SEQ, 0, 0, tiled=True).reshape(-1, 128)


def body(doc_lengths, queries, key_states, value_states):
    tok = queries.shape[0]
    own = jnp.stack([key_states, value_states], axis=0)
    group = head_lengths(doc_lengths)
    one = from_behind(own, 1)
    group, one = lax.optimization_barrier((group, one))
    two = from_behind(one, 1)
    lengths = all_lengths(group)
    three = from_behind(two, 1)
    four = from_behind(two[:, tok // 2 :], 2)
    base = jnp.reshape(lax.axis_index(SEQ) * tok, (1,)).astype(jnp.int32)
    m, l, acc = near(base, lengths, queries, own, one, two)
    return far(base, lengths, queries, three, four, m, l, acc)


def solution(mesh):
    finer = Mesh(mesh.devices.reshape(4, 8, 4, 2), SEQ + HEAD)
    return jax.shard_map(
        body,
        mesh=finer,
        in_specs=(P(SEQ + HEAD), P(SEQ, HEAD), P(SEQ, HEAD), P(SEQ, HEAD)),
        out_specs=P(SEQ, HEAD),
        check_vma=False,
    )
```

```python
import math

import jax
import jax.numpy as jnp
from jax import lax
from jax.experimental import pallas as pl
from jax.experimental.pallas import tpu as pltpu
from jax.sharding import Mesh
from jax.sharding import PartitionSpec as P

SEQ = ("seq_0", "seq_1")
HEAD = ("head_0", "head_1")

HD = 128
TILE = 256
KB = 384
HEADS_PER_DOT = 8
VL = 30
FAR_BELOW = -1e30
EXP2_SCALE = math.log2(math.e) / math.sqrt(HD)
NT = (((1,), (1,)), ((), ()))
NN = (((1,), (0,)), ((), ()))


def fill_ends(lengths_ref, ends_ref):
    docs = lengths_ref.shape[0]
    lengths = lengths_ref[...]
    order = lax.broadcasted_iota(jnp.int32, lengths.shape, 0)
    lane = lax.broadcasted_iota(jnp.int32, lengths.shape, 1)
    for part in range(docs // 128):
        kept = jnp.where(order <= lane + part * 128, lengths, 0)
        ends_ref[:, part * 128 : (part + 1) * 128] = jnp.sum(kept, axis=0, keepdims=True)


def place_tiles(base, lengths_ref, ends_ref, starts_ref, low_ref, high_ref):
    fill_ends(lengths_ref, ends_ref)
    ends = ends_ref[...]
    for t in range(starts_ref.shape[0]):
        pos = base + t * TILE + lax.broadcasted_iota(jnp.int32, (TILE, ends.shape[1]), 0)
        starts = jnp.max(jnp.where(ends <= pos, ends, 0), axis=1, keepdims=True)
        starts_ref[t] = jnp.broadcast_to(starts, (TILE, 128))
        low_ref[t] = jnp.min(starts)
        high_ref[t] = jnp.max(starts)


def take_tile(q_ref, t, qs_ref):
    rows = pl.ds(pl.multiple_of(t * TILE, TILE), TILE)
    for h in range(q_ref.shape[1] // HD):
        qs_ref[h * TILE : (h + 1) * TILE, :] = q_ref[rows, h * HD : (h + 1) * HD]


def accumulate(qs_ref, k_ref, v_ref, row, mask, m_ref, l_ref, acc_ref, fresh):
    rows_all = qs_ref.shape[0]
    step = HEADS_PER_DOT * TILE
    keys = k_ref[pl.ds(row, KB), :]
    values = v_ref[pl.ds(row, KB), :]
    for first in range(0, rows_all, step):
        rows = slice(first, first + step)
        scores = lax.dot_general(qs_ref[rows], keys, NT, preferred_element_type=jnp.float32)
        if mask is not None:
            scores = jnp.where(mask, scores.reshape(HEADS_PER_DOT, TILE, KB), FAR_BELOW).reshape(step, KB)
        top = jnp.max(scores, axis=1, keepdims=True)
        if not fresh:
            old = m_ref[rows]
            new = jnp.maximum(old, top)
            shrink = jnp.exp2((old - new) * EXP2_SCALE)
        else:
            new = jnp.broadcast_to(top, (step, 128))
        m_ref[rows] = new
        parts = [
            jnp.exp2((scores[:, c : c + 128] - new) * EXP2_SCALE) for c in range(0, KB, 128)
        ]
        total = parts[0]
        for part in parts[1:]:
            total = total + part
        weights = jnp.concatenate([part.astype(jnp.bfloat16) for part in parts], axis=1)
        update = lax.dot_general(weights, values, NN, preferred_element_type=jnp.float32)
        if not fresh:
            total = total + l_ref[rows] * shrink
            update = update + acc_ref[rows] * shrink
        l_ref[rows] = total
        acc_ref[rows] = update


def visible(first_pos, key_pos, starts, diagonal):
    key = key_pos + lax.broadcasted_iota(jnp.int32, (TILE, KB), 1)
    seen = key >= starts
    if diagonal:
        seen = seen & (key <= first_pos + lax.broadcasted_iota(jnp.int32, (TILE, KB), 0))
    return seen


def spread_copies(blocks, k_ref, v_ref, sems):
    copies = []
    for i, (src, row) in enumerate(blocks):
        rows = pl.ds(row, src.shape[1])
        copies += [
            pltpu.make_async_copy(src.at[0], k_ref.at[rows], sems.at[2 * i]),
            pltpu.make_async_copy(src.at[1], v_ref.at[rows], sems.at[2 * i + 1]),
        ]
    return copies


def near_kernel(base_ref, lengths_ref, q_ref, kv0_ref, kv1_ref, kv2_ref,
                m_out, l_out, acc_out, k_ref, v_ref, qs_ref, ends_ref, starts_ref, low_ref, high_ref, sems):
    tok = kv0_ref.shape[1]
    copies = spread_copies(
        [(kv2_ref, 0), (kv1_ref, tok), (kv0_ref, 2 * tok)], k_ref, v_ref, sems
    )
    for copy in copies:
        copy.start()
    base = base_ref[0]
    place_tiles(base, lengths_ref, ends_ref, starts_ref, low_ref, high_ref)
    kv_base = base - 2 * tok
    for copy in copies:
        copy.wait()

    def tile(t, _):
        first_pos = base + t * TILE
        low = low_ref[t]
        high = high_ref[t]
        take_tile(q_ref, t, qs_ref)
        m_ref, l_ref, acc_ref = m_out.at[t], l_out.at[t], acc_out.at[t]
        last = (2 * tok + (t + 1) * TILE - 1) // KB
        lowest = jnp.maximum(low - kv_base, 0) // KB
        row = pl.multiple_of(last * KB, KB)
        mask = visible(first_pos, kv_base + row, starts_ref[t][:, :1], True)
        accumulate(qs_ref, k_ref, v_ref, row, mask, m_ref, l_ref, acc_ref, True)

        def block(i, _):
            row = pl.multiple_of((last - 1 - i) * KB, KB)
            key_pos = kv_base + row

            clear = (key_pos >= high) & (key_pos + KB <= first_pos + 1)

            @pl.when(clear)
            def _():
                accumulate(qs_ref, k_ref, v_ref, row, None, m_ref, l_ref, acc_ref, False)

            @pl.when(jnp.logical_not(clear))
            def _():
                mask = visible(first_pos, key_pos, starts_ref[t][:, :1], True)
                accumulate(qs_ref, k_ref, v_ref, row, mask, m_ref, l_ref, acc_ref, False)

            return 0

        lax.fori_loop(0, last - lowest, block, 0)
        return 0

    lax.fori_loop(0, q_ref.shape[0] // TILE, tile, 0)


def far_kernel(base_ref, lengths_ref, q_ref, kv3_ref, kv4_ref, m_in, l_in, acc_in,
               out_ref, k_ref, v_ref, qs_ref, ends_ref, starts_ref, low_ref, high_ref, m_ref, l_ref, acc_ref, sems):
    tok = kv3_ref.shape[1]
    half = kv4_ref.shape[1]
    copies = spread_copies([(kv4_ref, 0), (kv3_ref, half)], k_ref, v_ref, sems)
    for copy in copies:
        copy.start()
    base = base_ref[0]
    place_tiles(base, lengths_ref, ends_ref, starts_ref, low_ref, high_ref)
    top_pos = base - 2 * tok
    kv_base = top_pos - tok - half
    for copy in copies:
        copy.wait()
    heads = q_ref.shape[1] // HD
    count = k_ref.shape[0] // KB

    def tile(t, _):
        first_pos = base + t * TILE
        low = low_ref[t]
        high = high_ref[t]
        q_rows = pl.multiple_of(t * TILE, TILE)

        def finish(m_now, l_now, acc_now):
            for h in range(heads):
                rows = slice(h * TILE, (h + 1) * TILE)
                total = jnp.sum(l_now[rows], axis=1, keepdims=True)
                out_ref[pl.ds(q_rows, TILE), h * HD : (h + 1) * HD] = (
                    acc_now[rows] * (1.0 / total)
                ).astype(out_ref.dtype)

        @pl.when(low >= top_pos)
        def _():
            finish(m_in.at[t], l_in.at[t], acc_in.at[t])

        @pl.when(low < top_pos)
        def _():
            take_tile(q_ref, t, qs_ref)
            m_ref[...] = m_in[t]
            l_ref[...] = l_in[t]
            acc_ref[...] = acc_in[t]
            lowest = jnp.maximum(low - kv_base, 0) // KB

            def block(i, _):
                row = pl.multiple_of((count - 1 - i) * KB, KB)
                key_pos = kv_base + row

                @pl.when(key_pos >= high)
                def _():
                    accumulate(qs_ref, k_ref, v_ref, row, None, m_ref, l_ref, acc_ref, False)

                @pl.when(key_pos < high)
                def _():
                    mask = visible(first_pos, key_pos, starts_ref[t][:, :1], False)
                    accumulate(qs_ref, k_ref, v_ref, row, mask, m_ref, l_ref, acc_ref, False)

                return 0

            lax.fori_loop(0, count - lowest, block, 0)
            finish(m_ref, l_ref, acc_ref)

        return 0

    lax.fori_loop(0, q_ref.shape[0] // TILE, tile, 0)


VM = pl.BlockSpec(memory_space=pltpu.VMEM)
SM = pl.BlockSpec(memory_space=pltpu.SMEM)
ANY = pl.BlockSpec(memory_space=pl.ANY)


def near(base, lengths, q, kv0, kv1, kv2):
    tok, width = q.shape
    tiles, rows = tok // TILE, width // HD * TILE
    state = jax.ShapeDtypeStruct((tiles, rows, 128), jnp.float32)
    return pl.pallas_call(
        near_kernel,
        out_shape=(state,) * 3,
        in_specs=[SM, VM, VM, ANY, ANY, ANY],
        out_specs=(VM,) * 3,
        scratch_shapes=[
            pltpu.VMEM((3 * tok, HD), jnp.bfloat16),
            pltpu.VMEM((3 * tok, HD), jnp.bfloat16),
            pltpu.VMEM((rows, HD), jnp.bfloat16),
            pltpu.VMEM((1, lengths.shape[0]), jnp.int32),
            pltpu.VMEM((tok // TILE, TILE, 128), jnp.int32),
            pltpu.SMEM((tok // TILE,), jnp.int32),
            pltpu.SMEM((tok // TILE,), jnp.int32),
            pltpu.SemaphoreType.DMA((6,)),
        ],
        compiler_params=pltpu.CompilerParams(vmem_limit_bytes=VL << 20),
        cost_estimate=pl.CostEstimate(flops=8_000_000_000, bytes_accessed=16 << 20, transcendentals=0),
        name="near",
    )(base, lengths, q, kv0, kv1, kv2)


def far(base, lengths, q, kv3, kv4, m, l, acc):
    tok, width = q.shape
    rows = width // HD * TILE
    return pl.pallas_call(
        far_kernel,
        out_shape=jax.ShapeDtypeStruct(q.shape, q.dtype),
        in_specs=[SM, VM, VM, ANY, ANY, VM, VM, VM],
        out_specs=VM,
        scratch_shapes=[
            pltpu.VMEM((tok + tok // 2, HD), jnp.bfloat16),
            pltpu.VMEM((tok + tok // 2, HD), jnp.bfloat16),
            pltpu.VMEM((rows, HD), jnp.bfloat16),
            pltpu.VMEM((1, lengths.shape[0]), jnp.int32),
            pltpu.VMEM((tok // TILE, TILE, 128), jnp.int32),
            pltpu.SMEM((tok // TILE,), jnp.int32),
            pltpu.SMEM((tok // TILE,), jnp.int32),
            pltpu.VMEM((rows, 128), jnp.float32),
            pltpu.VMEM((rows, 128), jnp.float32),
            pltpu.VMEM((rows, 128), jnp.float32),
            pltpu.SemaphoreType.DMA((4,)),
        ],
        compiler_params=pltpu.CompilerParams(vmem_limit_bytes=VL << 20),
        cost_estimate=pl.CostEstimate(flops=2_000_000_000, bytes_accessed=16 << 20, transcendentals=0),
        name="far",
    )(base, lengths, q, kv3, kv4, m, l, acc)


def from_behind(value, steps):
    count = lax.axis_size(SEQ)
    return lax.ppermute(value, SEQ, [(source, source + steps) for source in range(count - steps)])


def head_lengths(doc_lengths):
    heads = lax.axis_size(HEAD)
    per_head = doc_lengths.shape[0]
    rows = heads * per_head
    order = lax.broadcasted_iota(jnp.int32, (rows, 128), 0)
    mine = jnp.zeros((rows, 128), jnp.int32)
    for i in range(per_head):
        mine = jnp.where(order == lax.axis_index(HEAD) * per_head + i, doc_lengths[i], mine)
    return lax.psum(mine, HEAD)


def all_lengths(group):
    shards = lax.axis_size(SEQ)
    spread = jnp.broadcast_to(group[None], (shards, *group.shape))
    return lax.all_to_all(spread, SEQ, 0, 0, tiled=True).reshape(-1, 128)


def body(doc_lengths, queries, key_states, value_states):
    tok = queries.shape[0]
    own = jnp.stack([key_states, value_states], axis=0)
    group = head_lengths(doc_lengths)
    one = from_behind(own, 1)
    group, one = lax.optimization_barrier((group, one))
    two = from_behind(one, 1)
    lengths = all_lengths(group)
    three = from_behind(two, 1)
    four = from_behind(two[:, tok // 2 :], 2)
    base = jnp.reshape(lax.axis_index(SEQ) * tok, (1,)).astype(jnp.int32)
    m, l, acc = near(base, lengths, queries, own, one, two)
    return far(base, lengths, queries, three, four, m, l, acc)


def solution(mesh):
    finer = Mesh(mesh.devices.reshape(4, 8, 4, 2), SEQ + HEAD)
    return jax.shard_map(
        body,
        mesh=finer,
        in_specs=(P(SEQ + HEAD), P(SEQ, HEAD), P(SEQ, HEAD), P(SEQ, HEAD)),
        out_specs=P(SEQ, HEAD),
        check_vma=False,
    )
```

```python
import math

import jax
import jax.numpy as jnp
from jax import lax
from jax.experimental import pallas as pl
from jax.experimental.pallas import tpu as pltpu
from jax.sharding import Mesh
from jax.sharding import PartitionSpec as P

SEQ = ("seq_0", "seq_1")
HEAD = ("head_0", "head_1")

HD = 128
TILE = 256
KB = 384
HEADS_PER_DOT = 8
VL = 30
FAR_BELOW = -1e30
EXP2_SCALE = math.log2(math.e) / math.sqrt(HD)
NT = (((1,), (1,)), ((), ()))
NN = (((1,), (0,)), ((), ()))


def fill_ends(lengths_ref, ends_ref):
    docs = lengths_ref.shape[0]
    lengths = lengths_ref[...]
    order = lax.broadcasted_iota(jnp.int32, lengths.shape, 0)
    lane = lax.broadcasted_iota(jnp.int32, lengths.shape, 1)
    for part in range(docs // 128):
        kept = jnp.where(order <= lane + part * 128, lengths, 0)
        ends_ref[:, part * 128 : (part + 1) * 128] = jnp.sum(kept, axis=0, keepdims=True)


def place_tiles(base, lengths_ref, ends_ref, starts_ref, low_ref, high_ref):
    fill_ends(lengths_ref, ends_ref)
    ends = ends_ref[...]
    for t in range(starts_ref.shape[0]):
        pos = base + t * TILE + lax.broadcasted_iota(jnp.int32, (TILE, ends.shape[1]), 0)
        starts = jnp.max(jnp.where(ends <= pos, ends, 0), axis=1, keepdims=True)
        starts_ref[t] = jnp.broadcast_to(starts, (TILE, 128))
        low_ref[t] = jnp.min(starts)
        high_ref[t] = jnp.max(starts)


def take_tile(q_ref, t, qs_ref):
    rows = pl.ds(pl.multiple_of(t * TILE, TILE), TILE)
    for h in range(q_ref.shape[1] // HD):
        qs_ref[h * TILE : (h + 1) * TILE, :] = q_ref[rows, h * HD : (h + 1) * HD]


def accumulate(qs_ref, k_ref, v_ref, row, mask, m_ref, l_ref, acc_ref, fresh):
    rows_all = qs_ref.shape[0]
    step = HEADS_PER_DOT * TILE
    keys = k_ref[pl.ds(row, KB), :]
    values = v_ref[pl.ds(row, KB), :]
    for first in range(0, rows_all, step):
        rows = slice(first, first + step)
        scores = lax.dot_general(qs_ref[rows], keys, NT, preferred_element_type=jnp.float32)
        if mask is not None:
            scores = jnp.where(mask, scores.reshape(HEADS_PER_DOT, TILE, KB), FAR_BELOW).reshape(step, KB)
        top = jnp.max(scores, axis=1, keepdims=True)
        if not fresh:
            old = m_ref[rows]
            new = jnp.maximum(old, top)
            shrink = jnp.exp2((old - new) * EXP2_SCALE)
        else:
            new = jnp.broadcast_to(top, (step, 128))
        m_ref[rows] = new
        parts = [
            jnp.exp2((scores[:, c : c + 128] - new) * EXP2_SCALE) for c in range(0, KB, 128)
        ]
        total = parts[0]
        for part in parts[1:]:
            total = total + part
        weights = jnp.concatenate([part.astype(jnp.bfloat16) for part in parts], axis=1)
        update = lax.dot_general(weights, values, NN, preferred_element_type=jnp.float32)
        if not fresh:
            total = total + l_ref[rows] * shrink
            update = update + acc_ref[rows] * shrink
        l_ref[rows] = total
        acc_ref[rows] = update


def visible(first_pos, key_pos, starts, diagonal):
    key = key_pos + lax.broadcasted_iota(jnp.int32, (TILE, KB), 1)
    seen = key >= starts
    if diagonal:
        seen = seen & (key <= first_pos + lax.broadcasted_iota(jnp.int32, (TILE, KB), 0))
    return seen


def spread_copies(blocks, k_ref, v_ref, sems):
    copies = []
    for i, (src, row) in enumerate(blocks):
        rows = pl.ds(row, src.shape[1])
        copies += [
            pltpu.make_async_copy(src.at[0], k_ref.at[rows], sems.at[2 * i]),
            pltpu.make_async_copy(src.at[1], v_ref.at[rows], sems.at[2 * i + 1]),
        ]
    return copies


def near_kernel(base_ref, lengths_ref, q_hbm, kv0_ref, kv1_ref, kv2_ref,
                m_out, l_out, acc_out, k_ref, v_ref, q_ref, qs_ref, ends_ref, starts_ref, low_ref, high_ref, sems):
    tok = kv0_ref.shape[1]
    copies = spread_copies(
        [(kv2_ref, 0), (kv1_ref, tok), (kv0_ref, 2 * tok)], k_ref, v_ref, sems
    )
    copies.append(pltpu.make_async_copy(q_hbm, q_ref, sems.at[len(copies)]))
    for copy in copies:
        copy.start()
    base = base_ref[0]
    place_tiles(base, lengths_ref, ends_ref, starts_ref, low_ref, high_ref)
    kv_base = base - 2 * tok
    for copy in copies:
        copy.wait()

    def tile(t, _):
        first_pos = base + t * TILE
        low = low_ref[t]
        high = high_ref[t]
        take_tile(q_ref, t, qs_ref)
        m_ref, l_ref, acc_ref = m_out.at[t], l_out.at[t], acc_out.at[t]
        last = (2 * tok + (t + 1) * TILE - 1) // KB
        lowest = jnp.maximum(low - kv_base, 0) // KB
        row = pl.multiple_of(last * KB, KB)
        mask = visible(first_pos, kv_base + row, starts_ref[t][:, :1], True)
        accumulate(qs_ref, k_ref, v_ref, row, mask, m_ref, l_ref, acc_ref, True)

        def block(i, _):
            row = pl.multiple_of((last - 1 - i) * KB, KB)
            key_pos = kv_base + row

            clear = (key_pos >= high) & (key_pos + KB <= first_pos + 1)

            @pl.when(clear)
            def _():
                accumulate(qs_ref, k_ref, v_ref, row, None, m_ref, l_ref, acc_ref, False)

            @pl.when(jnp.logical_not(clear))
            def _():
                mask = visible(first_pos, key_pos, starts_ref[t][:, :1], True)
                accumulate(qs_ref, k_ref, v_ref, row, mask, m_ref, l_ref, acc_ref, False)

            return 0

        lax.fori_loop(0, last - lowest, block, 0)
        return 0

    lax.fori_loop(0, q_ref.shape[0] // TILE, tile, 0)


def far_kernel(base_ref, lengths_ref, q_hbm, far_ref, m_in, l_in, acc_in,
               out_ref, k_ref, v_ref, q_ref, qs_ref, ends_ref, starts_ref, low_ref, high_ref, m_ref, l_ref, acc_ref, sems):
    tok = q_ref.shape[0]
    half = far_ref.shape[1] - tok
    copies = spread_copies([(far_ref, 0)], k_ref, v_ref, sems)
    copies.append(pltpu.make_async_copy(q_hbm, q_ref, sems.at[len(copies)]))
    for copy in copies:
        copy.start()
    base = base_ref[0]
    place_tiles(base, lengths_ref, ends_ref, starts_ref, low_ref, high_ref)
    top_pos = base - 2 * tok
    kv_base = top_pos - tok - half
    for copy in copies:
        copy.wait()
    heads = q_ref.shape[1] // HD
    count = k_ref.shape[0] // KB

    def tile(t, _):
        first_pos = base + t * TILE
        low = low_ref[t]
        high = high_ref[t]
        q_rows = pl.multiple_of(t * TILE, TILE)

        def finish(m_now, l_now, acc_now):
            for h in range(heads):
                rows = slice(h * TILE, (h + 1) * TILE)
                total = jnp.sum(l_now[rows], axis=1, keepdims=True)
                out_ref[pl.ds(q_rows, TILE), h * HD : (h + 1) * HD] = (
                    acc_now[rows] * (1.0 / total)
                ).astype(out_ref.dtype)

        @pl.when(low >= top_pos)
        def _():
            finish(m_in.at[t], l_in.at[t], acc_in.at[t])

        @pl.when(low < top_pos)
        def _():
            take_tile(q_ref, t, qs_ref)
            m_ref[...] = m_in[t]
            l_ref[...] = l_in[t]
            acc_ref[...] = acc_in[t]
            lowest = jnp.maximum(low - kv_base, 0) // KB

            def block(i, _):
                row = pl.multiple_of((count - 1 - i) * KB, KB)
                key_pos = kv_base + row

                @pl.when(key_pos >= high)
                def _():
                    accumulate(qs_ref, k_ref, v_ref, row, None, m_ref, l_ref, acc_ref, False)

                @pl.when(key_pos < high)
                def _():
                    mask = visible(first_pos, key_pos, starts_ref[t][:, :1], False)
                    accumulate(qs_ref, k_ref, v_ref, row, mask, m_ref, l_ref, acc_ref, False)

                return 0

            lax.fori_loop(0, count - lowest, block, 0)
            finish(m_ref, l_ref, acc_ref)

        return 0

    lax.fori_loop(0, q_ref.shape[0] // TILE, tile, 0)


VM = pl.BlockSpec(memory_space=pltpu.VMEM)
SM = pl.BlockSpec(memory_space=pltpu.SMEM)
ANY = pl.BlockSpec(memory_space=pl.ANY)
HB = pl.BlockSpec(memory_space=pltpu.HBM)


def near(base, lengths, q, kv0, kv1, kv2):
    tok, width = q.shape
    tiles, rows = tok // TILE, width // HD * TILE
    state = jax.ShapeDtypeStruct((tiles, rows, 128), jnp.float32)
    return pl.pallas_call(
        near_kernel,
        out_shape=(state,) * 3,
        in_specs=[SM, VM, HB, ANY, ANY, ANY],
        out_specs=(VM,) * 3,
        scratch_shapes=[
            pltpu.VMEM((3 * tok, HD), jnp.bfloat16),
            pltpu.VMEM((3 * tok, HD), jnp.bfloat16),
            pltpu.VMEM(q.shape, q.dtype),
            pltpu.VMEM((rows, HD), jnp.bfloat16),
            pltpu.VMEM((1, lengths.shape[0]), jnp.int32),
            pltpu.VMEM((tok // TILE, TILE, 128), jnp.int32),
            pltpu.SMEM((tok // TILE,), jnp.int32),
            pltpu.SMEM((tok // TILE,), jnp.int32),
            pltpu.SemaphoreType.DMA((7,)),
        ],
        compiler_params=pltpu.CompilerParams(vmem_limit_bytes=VL << 20),
        cost_estimate=pl.CostEstimate(flops=8_000_000_000, bytes_accessed=16 << 20, transcendentals=0),
        name="near",
    )(base, lengths, q, kv0, kv1, kv2)


def far(base, lengths, q, kv_far, m, l, acc):
    tok, width = q.shape
    rows = width // HD * TILE
    return pl.pallas_call(
        far_kernel,
        out_shape=jax.ShapeDtypeStruct(q.shape, q.dtype),
        in_specs=[SM, VM, HB, ANY, VM, VM, VM],
        out_specs=VM,
        scratch_shapes=[
            pltpu.VMEM((tok + tok // 2, HD), jnp.bfloat16),
            pltpu.VMEM((tok + tok // 2, HD), jnp.bfloat16),
            pltpu.VMEM(q.shape, q.dtype),
            pltpu.VMEM((rows, HD), jnp.bfloat16),
            pltpu.VMEM((1, lengths.shape[0]), jnp.int32),
            pltpu.VMEM((tok // TILE, TILE, 128), jnp.int32),
            pltpu.SMEM((tok // TILE,), jnp.int32),
            pltpu.SMEM((tok // TILE,), jnp.int32),
            pltpu.VMEM((rows, 128), jnp.float32),
            pltpu.VMEM((rows, 128), jnp.float32),
            pltpu.VMEM((rows, 128), jnp.float32),
            pltpu.SemaphoreType.DMA((3,)),
        ],
        compiler_params=pltpu.CompilerParams(vmem_limit_bytes=VL << 20),
        cost_estimate=pl.CostEstimate(flops=2_000_000_000, bytes_accessed=16 << 20, transcendentals=0),
        name="far",
    )(base, lengths, q, kv_far, m, l, acc)


def from_behind(value, steps):
    count = lax.axis_size(SEQ)
    return lax.ppermute(value, SEQ, [(source, source + steps) for source in range(count - steps)])


def head_lengths(doc_lengths):
    heads = lax.axis_size(HEAD)
    per_head = doc_lengths.shape[0]
    rows = heads * per_head
    order = lax.broadcasted_iota(jnp.int32, (rows, 128), 0)
    mine = jnp.zeros((rows, 128), jnp.int32)
    for i in range(per_head):
        mine = jnp.where(order == lax.axis_index(HEAD) * per_head + i, doc_lengths[i], mine)
    return lax.psum(mine, HEAD)


def all_lengths(group):
    shards = lax.axis_size(SEQ)
    spread = jnp.broadcast_to(group[None], (shards, *group.shape))
    return lax.all_to_all(spread, SEQ, 0, 0, tiled=True).reshape(-1, 128)


def body(doc_lengths, queries, key_states, value_states):
    tok = queries.shape[0]
    own = jnp.stack([key_states, value_states], axis=0)
    group = head_lengths(doc_lengths)
    one = from_behind(own, 1)
    group, one = lax.optimization_barrier((group, one))
    two = from_behind(one, 1)
    lengths = all_lengths(group)
    beyond = from_behind(jnp.concatenate([two[:, tok // 2 :], one], axis=1), 2)
    base = jnp.reshape(lax.axis_index(SEQ) * tok, (1,)).astype(jnp.int32)
    m, l, acc = near(base, lengths, queries, own, one, two)
    return far(base, lengths, queries, beyond, m, l, acc)


def solution(mesh):
    finer = Mesh(mesh.devices.reshape(4, 8, 4, 2), SEQ + HEAD)
    return jax.shard_map(
        body,
        mesh=finer,
        in_specs=(P(SEQ + HEAD), P(SEQ, HEAD), P(SEQ, HEAD), P(SEQ, HEAD)),
        out_specs=P(SEQ, HEAD),
        check_vma=False,
    )
```

```python
import math

import jax
import jax.numpy as jnp
from jax import lax
from jax.experimental import pallas as pl
from jax.experimental.pallas import tpu as pltpu
from jax.sharding import Mesh
from jax.sharding import PartitionSpec as P

SEQ = ("seq_0", "seq_1")
HEAD = ("head_0", "head_1")

HD = 128
TILE = 256
KB = 384
HEADS_PER_DOT = 8
VL = 30
FAR_BELOW = -1e30
EXP2_SCALE = math.log2(math.e) / math.sqrt(HD)
NT = (((1,), (1,)), ((), ()))
NN = (((1,), (0,)), ((), ()))


def fill_ends(lengths_ref, ends_ref):
    docs = lengths_ref.shape[0]
    lengths = lengths_ref[...]
    order = lax.broadcasted_iota(jnp.int32, lengths.shape, 0)
    lane = lax.broadcasted_iota(jnp.int32, lengths.shape, 1)
    for part in range(docs // 128):
        kept = jnp.where(order <= lane + part * 128, lengths, 0)
        ends_ref[:, part * 128 : (part + 1) * 128] = jnp.sum(kept, axis=0, keepdims=True)


def place_tiles(base, lengths_ref, ends_ref, starts_ref, low_ref, high_ref):
    fill_ends(lengths_ref, ends_ref)
    ends = ends_ref[...]
    for t in range(starts_ref.shape[0]):
        pos = base + t * TILE + lax.broadcasted_iota(jnp.int32, (TILE, ends.shape[1]), 0)
        starts = jnp.max(jnp.where(ends <= pos, ends, 0), axis=1, keepdims=True)
        starts_ref[t] = jnp.broadcast_to(starts, (TILE, 128))
        low_ref[t] = jnp.min(starts)
        high_ref[t] = jnp.max(starts)


def take_tile(q_ref, t, qs_ref):
    rows = pl.ds(pl.multiple_of(t * TILE, TILE), TILE)
    for h in range(q_ref.shape[1] // HD):
        qs_ref[h * TILE : (h + 1) * TILE, :] = q_ref[rows, h * HD : (h + 1) * HD]


def accumulate(qs_ref, k_ref, v_ref, row, mask, m_ref, l_ref, acc_ref, fresh):
    rows_all = qs_ref.shape[0]
    step = HEADS_PER_DOT * TILE
    keys = k_ref[pl.ds(row, KB), :]
    values = v_ref[pl.ds(row, KB), :]
    for first in range(0, rows_all, step):
        rows = slice(first, first + step)
        scores = lax.dot_general(qs_ref[rows], keys, NT, preferred_element_type=jnp.float32)
        if mask is not None:
            scores = jnp.where(mask, scores.reshape(HEADS_PER_DOT, TILE, KB), FAR_BELOW).reshape(step, KB)
        top = jnp.max(scores, axis=1, keepdims=True)
        if not fresh:
            old = m_ref[rows]
            new = jnp.maximum(old, top)
            shrink = jnp.exp2((old - new) * EXP2_SCALE)
        else:
            new = jnp.broadcast_to(top, (step, 128))
        m_ref[rows] = new
        parts = [
            jnp.exp2((scores[:, c : c + 128] - new) * EXP2_SCALE) for c in range(0, KB, 128)
        ]
        total = parts[0]
        for part in parts[1:]:
            total = total + part
        weights = jnp.concatenate([part.astype(jnp.bfloat16) for part in parts], axis=1)
        update = lax.dot_general(weights, values, NN, preferred_element_type=jnp.float32)
        if not fresh:
            total = total + l_ref[rows] * shrink
            update = update + acc_ref[rows] * shrink
        l_ref[rows] = total
        acc_ref[rows] = update


def visible(first_pos, key_pos, starts, diagonal):
    key = key_pos + lax.broadcasted_iota(jnp.int32, (TILE, KB), 1)
    seen = key >= starts
    if diagonal:
        seen = seen & (key <= first_pos + lax.broadcasted_iota(jnp.int32, (TILE, KB), 0))
    return seen


def spread_copies(blocks, k_ref, v_ref, sems):
    copies = []
    for i, (src, row) in enumerate(blocks):
        rows = pl.ds(row, src.shape[1])
        copies += [
            pltpu.make_async_copy(src.at[0], k_ref.at[rows], sems.at[2 * i]),
            pltpu.make_async_copy(src.at[1], v_ref.at[rows], sems.at[2 * i + 1]),
        ]
    return copies


def near_kernel(base_ref, lengths_ref, q_hbm, kv0_ref, kv1_ref, kv2_ref,
                m_out, l_out, acc_out, k_ref, v_ref, q_ref, qs_ref, ends_ref, starts_ref, low_ref, high_ref, sems):
    tok = kv0_ref.shape[1]
    copies = spread_copies(
        [(kv2_ref, 0), (kv1_ref, tok), (kv0_ref, 2 * tok)], k_ref, v_ref, sems
    )
    copies.append(pltpu.make_async_copy(q_hbm, q_ref, sems.at[len(copies)]))
    for copy in copies:
        copy.start()
    base = base_ref[0]
    place_tiles(base, lengths_ref, ends_ref, starts_ref, low_ref, high_ref)
    kv_base = base - 2 * tok
    for copy in copies:
        copy.wait()

    def tile(t, _):
        first_pos = base + t * TILE
        low = low_ref[t]
        high = high_ref[t]
        take_tile(q_ref, t, qs_ref)
        m_ref, l_ref, acc_ref = m_out.at[t], l_out.at[t], acc_out.at[t]
        last = (2 * tok + (t + 1) * TILE - 1) // KB
        lowest = jnp.maximum(low - kv_base, 0) // KB
        row = pl.multiple_of(last * KB, KB)
        mask = visible(first_pos, kv_base + row, starts_ref[t][:, :1], True)
        accumulate(qs_ref, k_ref, v_ref, row, mask, m_ref, l_ref, acc_ref, True)

        def block(i, _):
            row = pl.multiple_of((last - 1 - i) * KB, KB)
            key_pos = kv_base + row

            clear = (key_pos >= high) & (key_pos + KB <= first_pos + 1)

            @pl.when(clear)
            def _():
                accumulate(qs_ref, k_ref, v_ref, row, None, m_ref, l_ref, acc_ref, False)

            @pl.when(jnp.logical_not(clear))
            def _():
                mask = visible(first_pos, key_pos, starts_ref[t][:, :1], True)
                accumulate(qs_ref, k_ref, v_ref, row, mask, m_ref, l_ref, acc_ref, False)

            return 0

        lax.fori_loop(0, last - lowest, block, 0)
        return 0

    lax.fori_loop(0, q_ref.shape[0] // TILE, tile, 0)


def far_kernel(base_ref, lengths_ref, q_hbm, far_ref, m_in, l_in, acc_in,
               out_ref, k_ref, v_ref, q_ref, qs_ref, ends_ref, starts_ref, low_ref, high_ref, m_ref, l_ref, acc_ref, sems):
    tok = q_ref.shape[0]
    half = far_ref.shape[1] - tok
    copies = spread_copies([(far_ref, 0)], k_ref, v_ref, sems)
    copies.append(pltpu.make_async_copy(q_hbm, q_ref, sems.at[len(copies)]))
    for copy in copies:
        copy.start()
    base = base_ref[0]
    place_tiles(base, lengths_ref, ends_ref, starts_ref, low_ref, high_ref)
    top_pos = base - 2 * tok
    kv_base = top_pos - tok - half
    for copy in copies:
        copy.wait()
    heads = q_ref.shape[1] // HD
    count = k_ref.shape[0] // KB

    def tile(t, _):
        first_pos = base + t * TILE
        low = low_ref[t]
        high = high_ref[t]
        q_rows = pl.multiple_of(t * TILE, TILE)

        def finish(m_now, l_now, acc_now):
            for h in range(heads):
                rows = slice(h * TILE, (h + 1) * TILE)
                total = jnp.sum(l_now[rows], axis=1, keepdims=True)
                out_ref[pl.ds(q_rows, TILE), h * HD : (h + 1) * HD] = (
                    acc_now[rows] * (1.0 / total)
                ).astype(out_ref.dtype)

        @pl.when(low >= top_pos)
        def _():
            finish(m_in.at[t], l_in.at[t], acc_in.at[t])

        @pl.when(low < top_pos)
        def _():
            take_tile(q_ref, t, qs_ref)
            m_ref[...] = m_in[t]
            l_ref[...] = l_in[t]
            acc_ref[...] = acc_in[t]
            lowest = jnp.maximum(low - kv_base, 0) // KB

            def block(i, _):
                row = pl.multiple_of((count - 1 - i) * KB, KB)
                key_pos = kv_base + row

                @pl.when(key_pos >= high)
                def _():
                    accumulate(qs_ref, k_ref, v_ref, row, None, m_ref, l_ref, acc_ref, False)

                @pl.when(key_pos < high)
                def _():
                    mask = visible(first_pos, key_pos, starts_ref[t][:, :1], False)
                    accumulate(qs_ref, k_ref, v_ref, row, mask, m_ref, l_ref, acc_ref, False)

                return 0

            lax.fori_loop(0, count - lowest, block, 0)
            finish(m_ref, l_ref, acc_ref)

        return 0

    lax.fori_loop(0, q_ref.shape[0] // TILE, tile, 0)


VM = pl.BlockSpec(memory_space=pltpu.VMEM)
SM = pl.BlockSpec(memory_space=pltpu.SMEM)
ANY = pl.BlockSpec(memory_space=pl.ANY)
HB = pl.BlockSpec(memory_space=pltpu.HBM)


def near(base, lengths, q, kv0, kv1, kv2):
    tok, width = q.shape
    tiles, rows = tok // TILE, width // HD * TILE
    state = jax.ShapeDtypeStruct((tiles, rows, 128), jnp.float32)
    return pl.pallas_call(
        near_kernel,
        out_shape=(state,) * 3,
        in_specs=[SM, VM, HB, ANY, ANY, ANY],
        out_specs=(VM,) * 3,
        scratch_shapes=[
            pltpu.VMEM((3 * tok, HD), jnp.bfloat16),
            pltpu.VMEM((3 * tok, HD), jnp.bfloat16),
            pltpu.VMEM(q.shape, q.dtype),
            pltpu.VMEM((rows, HD), jnp.bfloat16),
            pltpu.VMEM((1, lengths.shape[0]), jnp.int32),
            pltpu.VMEM((tok // TILE, TILE, 128), jnp.int32),
            pltpu.SMEM((tok // TILE,), jnp.int32),
            pltpu.SMEM((tok // TILE,), jnp.int32),
            pltpu.SemaphoreType.DMA((7,)),
        ],
        compiler_params=pltpu.CompilerParams(vmem_limit_bytes=VL << 20),
        cost_estimate=pl.CostEstimate(flops=8_000_000_000, bytes_accessed=16 << 20, transcendentals=0),
        name="near",
    )(base, lengths, q, kv0, kv1, kv2)


def far(base, lengths, q, kv_far, m, l, acc):
    tok, width = q.shape
    rows = width // HD * TILE
    return pl.pallas_call(
        far_kernel,
        out_shape=jax.ShapeDtypeStruct(q.shape, q.dtype),
        in_specs=[SM, VM, HB, ANY, VM, VM, VM],
        out_specs=VM,
        scratch_shapes=[
            pltpu.VMEM((tok + tok // 2, HD), jnp.bfloat16),
            pltpu.VMEM((tok + tok // 2, HD), jnp.bfloat16),
            pltpu.VMEM(q.shape, q.dtype),
            pltpu.VMEM((rows, HD), jnp.bfloat16),
            pltpu.VMEM((1, lengths.shape[0]), jnp.int32),
            pltpu.VMEM((tok // TILE, TILE, 128), jnp.int32),
            pltpu.SMEM((tok // TILE,), jnp.int32),
            pltpu.SMEM((tok // TILE,), jnp.int32),
            pltpu.VMEM((rows, 128), jnp.float32),
            pltpu.VMEM((rows, 128), jnp.float32),
            pltpu.VMEM((rows, 128), jnp.float32),
            pltpu.SemaphoreType.DMA((3,)),
        ],
        compiler_params=pltpu.CompilerParams(vmem_limit_bytes=VL << 20),
        cost_estimate=pl.CostEstimate(flops=2_000_000_000, bytes_accessed=16 << 20, transcendentals=0),
        name="far",
    )(base, lengths, q, kv_far, m, l, acc)


def from_behind(value, steps):
    count = lax.axis_size(SEQ)
    return lax.ppermute(value, SEQ, [(source, source + steps) for source in range(count - steps)])


def head_lengths(doc_lengths):
    heads = lax.axis_size(HEAD)
    per_head = doc_lengths.shape[0]
    rows = heads * per_head
    order = lax.broadcasted_iota(jnp.int32, (rows, 128), 0)
    mine = jnp.zeros((rows, 128), jnp.int32)
    for i in range(per_head):
        mine = jnp.where(order == lax.axis_index(HEAD) * per_head + i, doc_lengths[i], mine)
    return lax.psum(mine, HEAD)


def all_lengths(group):
    shards = lax.axis_size(SEQ)
    spread = jnp.broadcast_to(group[None], (shards, *group.shape))
    return lax.all_to_all(spread, SEQ, 0, 0, tiled=True).reshape(-1, 128)


def body(doc_lengths, queries, key_states, value_states):
    tok = queries.shape[0]
    own = jnp.stack([key_states, value_states], axis=0)
    group = head_lengths(doc_lengths)
    one = from_behind(own, 1)
    group, one = lax.optimization_barrier((group, one))
    two = from_behind(own, 2)
    lengths = all_lengths(group)
    beyond = from_behind(jnp.concatenate([two[:, tok // 2 :], one], axis=1), 2)
    base = jnp.reshape(lax.axis_index(SEQ) * tok, (1,)).astype(jnp.int32)
    m, l, acc = near(base, lengths, queries, own, one, two)
    return far(base, lengths, queries, beyond, m, l, acc)


def solution(mesh):
    finer = Mesh(mesh.devices.reshape(4, 8, 4, 2), SEQ + HEAD)
    return jax.shard_map(
        body,
        mesh=finer,
        in_specs=(P(SEQ + HEAD), P(SEQ, HEAD), P(SEQ, HEAD), P(SEQ, HEAD)),
        out_specs=P(SEQ, HEAD),
        check_vma=False,
    )
```
